32 devices in a mesh: dp: 2 (over x), mp: 16 (over z, y, core).
Axes of the slice: x: 2, y: 2, z: 4, core: 2. Of those that a mesh axis runs over, the one named last changes fastest.
Arguments:
- base_rows: bfloat16 [256, 8192], P('dp', 'mp'), may hold values from -6 to 6
- layer_rows: bfloat16 [256, 8192], P('dp', 'mp'), may hold values from -6 to 6
- cross_weight: bfloat16 [8192, 8192], P(None, 'mp'), may hold values from -0.0625 to 0.0625
- cross_bias: float32 [8192], P('mp'), may hold values from -3 to 3
- upstream: bfloat16 [256, 8192], P('dp', 'mp'), may hold values from -6 to 6
Outputs:
- crossed: bfloat16 [256, 8192], P('dp', 'mp')
- grad_base: bfloat16 [256, 8192], P('dp', 'mp')
- grad_layer: bfloat16 [256, 8192], P('dp', 'mp')
- grad_weight: float32 [8192, 8192], P('dp', 'mp')
- grad_bias: float32 [8192], P('mp')
The draws below stay inside these ranges and needn't reach their ends.
All inputs are finite; a program needn't handle non-finite values.
Results may differ from the reference program's by a relative error of at most 0.0041.
Values may be sent and summed in bfloat16 or wider, within the bound.
No kernel may reach another device: no remote copies, remote signals or barrier semaphores. Data moves between devices by JAX's collectives and lax.ppermute only.
A program may use at most 128 MiB of HBM per device.

```python
import jax
import jax.numpy as jnp

D = 8192
BATCH = 256


def block_scale(key, extent, pieces, least, largest):
    level = 1.0
    for axis_at, blocks in pieces:
        heights = jax.random.uniform(jax.random.fold_in(jax.random.fold_in(key, 6), axis_at), (blocks,), jnp.float32, least / len(pieces), largest / len(pieces))
        level = level * jnp.repeat(jnp.exp(heights), extent[axis_at] // blocks).reshape((-1,) + (1,) * (len(extent) - 1 - axis_at))
    return level


def centred(rng, extent, spread, limit, split=(), dtype=jnp.bfloat16):
    array = jax.random.normal(rng, extent, jnp.float32) * spread
    if len(split) > 0:
        array = block_scale(rng, extent, split, -0.22, 0.18) * array
    return jnp.clip(array, min=-limit, max=limit).astype(dtype)


def setup_inputs(seed: int = 0) -> dict:
    splits = jax.random.split(jax.random.key(seed), 6)
    return {
        "base_rows": centred(splits[0], (BATCH, D), 1.0, 6.0, ((0, 2), (1, 16))),
        "layer_rows": centred(splits[1], (BATCH, D), 1.0, 6.0, ((0, 2), (1, 16))),
        "cross_weight": centred(splits[2], (D, D), D ** -0.5, 0.0625, ((1, 16),)),
        "cross_bias": centred(splits[3], (D,), 0.5, 3.0, ((0, 16),), jnp.float32),
        "upstream": centred(splits[4], (BATCH, D), 1.0, 6.0, ((0, 2), (1, 16))),
    }


def reference(base_rows, layer_rows, cross_weight, cross_bias, upstream):
    mixed = jnp.dot(layer_rows, cross_weight, preferred_element_type=jnp.float32) + cross_bias
    base = base_rows.astype(jnp.float32)
    crossed = (base * mixed + layer_rows.astype(jnp.float32)).astype(jnp.bfloat16)
    upper = upstream.astype(jnp.float32)
    delta = upper * base
    delta_low = delta.astype(jnp.bfloat16)
    grad_base = (upper * mixed).astype(jnp.bfloat16)
    back = jnp.dot(delta_low, cross_weight.T, preferred_element_type=jnp.float32)
    grad_layer = (upper + back).astype(jnp.bfloat16)
    scale = jnp.float32(BATCH) ** -0.5
    grad_weight = jnp.dot(layer_rows.T, delta_low, preferred_element_type=jnp.float32) * scale
    grad_bias = jnp.sum(delta, axis=0) * scale
    return crossed, grad_base, grad_layer, grad_weight, grad_bias
```

```python
import functools

import jax
import jax.numpy as jnp
from jax import lax
from jax.experimental import pallas as pl
from jax.experimental.pallas import tpu as pltpu
from jax.sharding import PartitionSpec as P


F32 = jnp.float32
BF16 = jnp.bfloat16


def _hop(x, axis, mask):
    size = lax.axis_size(axis)
    return lax.ppermute(x, axis, [(i, i ^ mask) for i in range(size)])


def _masks(n):
    bits = n.bit_length() - 1
    return [1 << b for b in range(1, bits - 1)] + [3 << (bits - 2)]


def _offset(v, masks):
    o = 0
    for i, mask in enumerate(masks):
        if v >> i & 1:
            o ^= mask
    return o


def _last_dim(v, dims):
    for d in range(dims):
        if v >> d & 1 and v >> ((d - 1) % dims) & 1:
            return d
    return v.bit_length() - 1


def _gather(x, masks):
    dims = len(masks)
    held = {0: x}
    for v in sorted(range(1, 1 << dims), key=lambda v: v.bit_count()):
        d = _last_dim(v, dims)
        held[v] = _hop(held[v ^ 1 << d], "mp", masks[d])
    return {_offset(v, masks): block for v, block in held.items()}


def _nt(a, b):
    return lax.dot_general(a, b, (((1,), (1,)), ((), ())), preferred_element_type=F32)


def _tn(a, b):
    return lax.dot_general(a, b, (((0,), (0,)), ((), ())), preferred_element_type=F32)


def _back_kernel(pair_ref, core_ref, base_ref, up_ref, w_ref, keep_ref, send_ref, delta_ref):
    cols = base_ref.shape[1]
    core = core_ref[0]

    @pl.when(pl.program_id(0) == 0)
    def _():
        delta_ref[...] = (up_ref[...].astype(F32) * base_ref[...].astype(F32)).astype(BF16)

    delta = delta_ref[...]
    mine = pl.multiple_of(core * cols, cols)
    other = pl.multiple_of((1 - core) * cols, cols)
    send_ref[0] = _nt(delta, w_ref[pl.ds(other, cols), :]).astype(BF16)
    keep_ref[0] = _nt(delta, w_ref[pl.ds(mine, cols), :]).astype(BF16)


def _back(base, up, w, pairs, core):
    rows, cols = base.shape
    half = w.shape[0] // (2 * cols)
    out = jax.ShapeDtypeStruct((half, rows, cols), BF16)
    whole = pl.BlockSpec((rows, cols), lambda j, p, c: (0, 0))
    return pl.pallas_call(
        _back_kernel,
        grid_spec=pltpu.PrefetchScalarGridSpec(
            num_scalar_prefetch=2,
            grid=(half,),
            in_specs=[whole, whole, pl.BlockSpec((2 * cols, cols), lambda j, p, c: (p[j], 0))],
            out_specs=[pl.BlockSpec((1, rows, cols), lambda j, p, c: (j, 0, 0))] * 2,
            scratch_shapes=[pltpu.VMEM((rows, cols), BF16)],
        ),
        out_shape=[out, out],
        cost_estimate=pl.CostEstimate(
            flops=2 * rows * w.size, bytes_accessed=2 * w.size, transcendentals=0
        ),
        name="back",
    )(pairs, core, base, up, w)


def _mixed_kernel(
    pair_ref, core_ref, even_ref, odd_ref, w_ref, bias_ref, base_ref, layer_ref, up_ref,
    crossed_ref, grad_ref, acc_ref,
):
    cols = base_ref.shape[1]
    core = core_ref[0]
    j = pl.program_id(0)
    mine = pl.multiple_of(core * cols, cols)
    other = pl.multiple_of((1 - core) * cols, cols)
    part = jnp.dot(even_ref[0], w_ref[pl.ds(mine, cols), :], preferred_element_type=F32)
    part += jnp.dot(odd_ref[0], w_ref[pl.ds(other, cols), :], preferred_element_type=F32)

    @pl.when(j == 0)
    def _():
        acc_ref[...] = part

    @pl.when(j > 0)
    def _():
        acc_ref[...] += part

    @pl.when(j == pl.num_programs(0) - 1)
    def _():
        mixed = acc_ref[...] + bias_ref[...]
        base = base_ref[...].astype(F32)
        crossed_ref[...] = (base * mixed + layer_ref[...].astype(F32)).astype(BF16)
        grad_ref[...] = (up_ref[...].astype(F32) * mixed).astype(BF16)


def _mixed(even, odd, w, bias, base, layer, up, pairs, core):
    half, rows, cols = even.shape
    out = jax.ShapeDtypeStruct((rows, cols), BF16)
    whole = pl.BlockSpec((rows, cols), lambda j, p, c: (0, 0))
    block = pl.BlockSpec((1, rows, cols), lambda j, p, c: (j, 0, 0))
    return pl.pallas_call(
        _mixed_kernel,
        grid_spec=pltpu.PrefetchScalarGridSpec(
            num_scalar_prefetch=2,
            grid=(half,),
            in_specs=[
                block,
                block,
                pl.BlockSpec((2 * cols, cols), lambda j, p, c: (p[j], 0)),
                pl.BlockSpec((1, cols), lambda j, p, c: (0, 0)),
                whole,
                whole,
                whole,
            ],
            out_specs=[whole, whole],
            scratch_shapes=[pltpu.VMEM((rows, cols), F32)],
        ),
        out_shape=[out, out],
        cost_estimate=pl.CostEstimate(
            flops=2 * rows * w.size, bytes_accessed=2 * w.size, transcendentals=0
        ),
        name="mixed",
    )(pairs, core, even, odd, w, bias.reshape(1, cols), base, layer, up)


def _weight_kernel(
    scale, first_ref, out_ref_index, core_ref, even_ref, odd_ref, even_far_ref, odd_far_ref,
    base_ref, up_ref, grad_ref, bias_ref, delta_ref, rows_ref,
):
    groups, rows, cols = base_ref.shape
    core = core_ref[0]

    @pl.when(pl.program_id(0) == 0)
    def _():
        total = jnp.zeros((1, cols), F32)
        for g in range(groups):
            delta = up_ref[g].astype(F32) * base_ref[g].astype(F32)
            delta_ref[g * rows : (g + 1) * rows, :] = delta.astype(BF16)
            total += jnp.sum(delta, axis=0, keepdims=True)
        bias_ref[...] = total * scale

    delta = delta_ref[...]
    for k, (near, far) in enumerate(((even_ref, even_far_ref), (odd_ref, odd_far_ref))):
        rows_ref[0:rows, :] = near[0]
        for g in range(groups - 1):
            rows_ref[(g + 1) * rows : (g + 2) * rows, :] = far[g, 0]
        at = pl.multiple_of((core if k == 0 else 1 - core) * cols, cols)
        grad_ref[pl.ds(at, cols), :] = _tn(rows_ref[...], delta) * scale


def _weight(even, odd, even_far, odd_far, base, up, first, places, core, scale):
    _, rows, cols = even.shape
    groups, steps = base.shape[0], even_far.shape[1]
    near = pl.BlockSpec((1, rows, cols), lambda j, f, o, c: (f[0] + j, 0, 0))
    far = pl.BlockSpec((groups - 1, 1, rows, cols), lambda j, f, o, c: (0, j, 0, 0))
    whole = pl.BlockSpec((groups, rows, cols), lambda j, f, o, c: (0, 0, 0))
    return pl.pallas_call(
        functools.partial(_weight_kernel, scale),
        grid_spec=pltpu.PrefetchScalarGridSpec(
            num_scalar_prefetch=3,
            grid=(steps,),
            in_specs=[near, near, far, far, whole, whole],
            out_specs=[
                pl.BlockSpec((2 * cols, cols), lambda j, f, o, c: (o[j], 0)),
                pl.BlockSpec((1, cols), lambda j, f, o, c: (0, 0)),
            ],
            scratch_shapes=[
                pltpu.VMEM((groups * rows, cols), BF16),
                pltpu.VMEM((groups * rows, cols), BF16),
            ],
        ),
        out_shape=[
            jax.ShapeDtypeStruct((2 * steps * cols, cols), F32),
            jax.ShapeDtypeStruct((1, cols), F32),
        ],
        cost_estimate=pl.CostEstimate(
            flops=4 * groups * rows * steps * cols * cols,
            bytes_accessed=8 * steps * cols * cols,
            transcendentals=0,
        ),
        name="weight",
    )(first, places, core, even, odd, even_far, odd_far, base, up)


def _stack(blocks):
    return jnp.stack(blocks)


def local(base_rows, layer_rows, cross_weight, cross_bias, upstream):
    groups, n = lax.axis_size("dp"), lax.axis_size("mp")
    d, m = lax.axis_index("dp"), lax.axis_index("mp")
    rows, cols = base_rows.shape
    half, share = n // 2, n // groups // 2
    masks = _masks(n)
    core = (m & 1).astype(jnp.int32).reshape(1)
    pairs = ((m >> 1) ^ jnp.arange(half, dtype=jnp.int32)).astype(jnp.int32)
    mine = (m >> 1) // share ^ d
    scale = float(rows * groups) ** -0.5

    blocks = _gather(layer_rows, masks)
    even = _stack([blocks[2 * j] for j in range(half)])
    odd = _hop(even, "mp", 1)

    base_far = [_hop(base_rows, "dp", t) for t in range(1, groups)]
    up_far = [_hop(upstream, "dp", t) for t in range(1, groups)]
    even_far = []
    for t in range(1, groups):
        start = (mine ^ t) * share
        even_far.append(_hop(lax.dynamic_slice_in_dim(even, start, share), "dp", t))
    even_far = _stack(even_far)
    odd_far = _hop(even_far, "mp", 1)

    keep, send = _back(base_rows, upstream, cross_weight, pairs, core)
    got = _hop(send, "mp", 1)
    held = [keep[j].astype(F32) + got[j].astype(F32) for j in range(half)]
    live = list(range(1 << len(masks)))
    for i, mask in enumerate(masks):
        leave = [v for v in live if v >> i & 1]
        live = [v for v in live if not v >> i & 1]
        came = _hop(_stack([held[_offset(v, masks) // 2].astype(BF16) for v in leave]), "mp", mask)
        for k, v in enumerate(leave):
            at = _offset(v ^ 1 << i, masks) // 2
            held[at] = held[at] + came[k].astype(F32)
    grad_layer = (upstream.astype(F32) + held[0]).astype(BF16)

    crossed, grad_base = _mixed(
        even, odd, cross_weight, cross_bias, base_rows, layer_rows, upstream, pairs, core
    )
    first = (mine * share).astype(jnp.int32).reshape(1)
    places = ((m >> 1) ^ (mine * share + jnp.arange(share, dtype=jnp.int32))) % share
    grad_weight, grad_bias = _weight(
        even, odd, even_far, odd_far, _stack([base_rows] + base_far), _stack([upstream] + up_far),
        first, places.astype(jnp.int32), core, scale,
    )
    return (crossed, grad_base, grad_layer, grad_weight, grad_bias.reshape(cols))


def solution(mesh):
    return jax.shard_map(
        local,
        mesh=mesh,
        in_specs=(P("dp", "mp"), P("dp", "mp"), P(None, "mp"), P("mp"), P("dp", "mp")),
        out_specs=(P("dp", "mp"), P("dp", "mp"), P("dp", "mp"), P("dp", "mp"), P("mp")),
        check_vma=False,
    )
```
